32 devices in a mesh: groups: 1, seq: 1, row: 16 (over z, y, core), col: 2 (over x).
Axes of the slice: x: 2, y: 2, z: 4, core: 2. Of those that a mesh axis runs over, the one named last changes fastest.
Arguments:
- paired_left: bfloat16 [512, 32, 512], P(('groups', 'seq', 'col'), None, 'row'), may hold values from -24 to 24
- paired_right: bfloat16 [512, 32, 512], P(('groups', 'seq', 'row'), None, 'col'), may hold values from -24 to 24
- unpaired_left: bfloat16 [1024, 32, 512], P(('groups', 'seq', 'col'), None, 'row'), may hold values from -24 to 24
- unpaired_right: bfloat16 [1024, 32, 512], P(('groups', 'seq', 'row'), None, 'col'), may hold values from -24 to 24
- out_weight: bfloat16 [1024, 128], replicated, may hold values from -0.1875 to 0.1875
- out_bias: float32 [128], replicated, may hold values from -6 to 6
- chain_lengths: int32 [12], P('groups'), may hold values from 1 to 128, 512 in all
- unpaired_depths: int32 [12], P('groups'), may hold values from 256 to 1024
Outputs:
- pair_update: bfloat16 [512, 512, 128], P(('groups', 'row'), ('col', 'seq'))
The draws below stay inside these ranges and needn't reach their ends.
Inputs may be any that keep to these rules, and one draw needn't show every extreme that they name: `chain_lengths`: chain lengths sum to 512. `unpaired_depths`: rows of the unpaired MSA at or beyond a chain's depth are padding.
All inputs are finite; a program needn't handle non-finite values.
Results may differ from the reference program's by a relative error of at most 0.0034.
Values may be sent and summed in bfloat16 or wider, within the bound.
A program may use at most 128 MiB of HBM per device.

```python
import math
import jax
import jax.numpy as jnp
import numpy as np
from jax import lax

C = 32
Z = 128
CHAINS = 12
S_P = 512
DMAX = 1024
N = 512
N_SEQ = 1


def place_ends(result, own_key, least, top_value):
    longest = result.shape.index(max(result.shape))
    spots = []
    for shift in (0, 1):
        where = [jax.random.randint(jax.random.fold_in(own_key, axis), (), 0, length) for axis, length in enumerate(result.shape)]
        where[longest] = (where[longest] + shift) % result.shape[longest]
        spots.append(tuple(where))
    return result.at[spots[0]].set(least).at[spots[1]].set(top_value)


def block_scale(key, shape, shards, least, high):
    level = 1.0
    for axis_at, parts in shards:
        steps = jax.random.uniform(jax.random.fold_in(jax.random.fold_in(key, 6), axis_at), (parts,), jnp.float32, least / len(shards), high / len(shards))
        level = level * jnp.repeat(jnp.exp(steps), shape[axis_at] // parts).reshape((-1,) + (1,) * (len(shape) - 1 - axis_at))
    return level


def length_profile(number_of, total, bound, skew):
    weights = [(1 << 20) // math.isqrt(rank ** skew) + 1 for rank in range(2, number_of + 1)]
    spare, given = total - bound - (number_of - 1), [1] * (number_of - 1)
    while spare > 0:
        free = [i for i in range(number_of - 1) if given[i] < bound]
        pool, left = sum([weights[i] for i in free]), spare
        for i in free:
            more = min(bound - given[i], max(1, left * weights[i] // pool), spare)
            given[i] = given[i] + more
            spare = spare - more
    return np.array([bound] + given)


def ragged_sizes(key, number_of, total, most, lean):
    if number_of == 2:
        one = jax.random.randint(key, (), max(1, total - most), min(most, total - 1) + 1)
        return jnp.stack([one, total - one])
    sizes = jnp.asarray(length_profile(number_of, total, most, lean), jnp.int32)
    couples = (number_of - 1) // 2
    source_of, taker = sizes[1:1 + 2 * couples:2], sizes[2:2 + 2 * couples:2]
    slack = jnp.minimum(source_of - 1, most - taker)
    moved = jax.random.randint(jax.random.fold_in(key, 1), (couples,), 0, 1 << 20) % (slack + 1)
    sizes = sizes.at[1:1 + 2 * couples:2].set(source_of - moved).at[2:2 + 2 * couples:2].set(taker + moved)
    return sizes[jax.random.permutation(jax.random.fold_in(key, 2), number_of)]


def scatter_about(own_key, shape, spread, bound, split=(), kind=jnp.bfloat16):
    factor_of = block_scale(own_key, shape, split, -0.22, 0.18) if split else 1.0
    values = jax.random.normal(own_key, shape, jnp.float32) * spread * factor_of
    return jnp.minimum(jnp.maximum(values, -bound), bound).astype(kind)


def setup_inputs(seed: int = 0, part: int = 0) -> dict:
    streams_of = jax.random.split(jax.random.key(seed), 9)
    part_keys = jax.random.split(jax.random.fold_in(streams_of[8], part), 9)
    paired_left = scatter_about(part_keys[0], (S_P, C, N), 4.0, 24.0, ((0, 2), (2, 16)))
    paired_right = scatter_about(part_keys[1], (S_P, C, N), 4.0, 24.0, ((0, 16), (2, 2)))
    unpaired_left = scatter_about(part_keys[2], (DMAX, C, N), 4.0, 24.0, ((0, 2), (2, 16)))
    unpaired_right = scatter_about(part_keys[3], (DMAX, C, N), 4.0, 24.0, ((0, 16), (2, 2)))
    out_weight = scatter_about(streams_of[4], (C * C, Z), (C * C) ** -0.5, 0.1875)
    out_bias = scatter_about(streams_of[5], (Z,), 1.0, 6.0, (), jnp.float32)
    chain_lengths = ragged_sizes(part_keys[6], CHAINS, N, N // 4, 1).astype(jnp.int32)
    unpaired_depths = place_ends(jax.random.randint(part_keys[7], (CHAINS,), DMAX // 4, DMAX + 1), jax.random.fold_in(part_keys[7], 1), DMAX // 4, DMAX).astype(jnp.int32)
    return {"paired_left": paired_left, "paired_right": paired_right, "unpaired_left": unpaired_left, "unpaired_right": unpaired_right, "out_weight": out_weight, "out_bias": out_bias, "chain_lengths": chain_lengths, "unpaired_depths": unpaired_depths}


def chain_tables(chain_lengths, unpaired_depths):
    positions = jnp.arange(N, dtype=jnp.int32)
    chain_ends = jnp.cumsum(chain_lengths).astype(jnp.int32)
    chain_of = jnp.sum((positions[:, None] >= chain_ends[None, :]).astype(jnp.int32), axis=1).astype(jnp.int32)
    onehot = chain_of[:, None] == jnp.arange(CHAINS, dtype=jnp.int32)[None, :]
    depth_of = jnp.sum(jnp.where(onehot, unpaired_depths[None, :], 0), axis=1).astype(jnp.int32)
    return chain_of, depth_of


def reference(paired_left, paired_right, unpaired_left, unpaired_right, out_weight, out_bias, chain_lengths, unpaired_depths):
    chain_of, depth_of = chain_tables(chain_lengths, unpaired_depths)
    free_ids = jnp.arange(DMAX, dtype=jnp.int32)
    live = (free_ids[:, None] < depth_of[None, :]).astype(unpaired_left.dtype)
    masked_left = unpaired_left * live[:, None, :]
    paired_group = S_P // N_SEQ
    free_group = DMAX // N_SEQ
    ref_rows = 8

    def one_block(block_index):
        offset = (block_index * ref_rows).astype(jnp.int32)
        chain_block = lax.dynamic_slice_in_dim(chain_of, offset, ref_rows, 0)
        depth_block = lax.dynamic_slice_in_dim(depth_of, offset, ref_rows, 0)
        same_chain = (chain_block[:, None] == chain_of[None, :]).astype(jnp.float32)
        summed = jnp.zeros((ref_rows, N, Z), jnp.float32)
        for group in range(N_SEQ):
            left_pair = lax.dynamic_slice_in_dim(paired_left[group * paired_group:(group + 1) * paired_group], offset, ref_rows, 2).astype(jnp.float32)
            right_pair = paired_right[group * paired_group:(group + 1) * paired_group].astype(jnp.float32)
            left_free = lax.dynamic_slice_in_dim(masked_left[group * free_group:(group + 1) * free_group], offset, ref_rows, 2).astype(jnp.float32)
            right_free = unpaired_right[group * free_group:(group + 1) * free_group].astype(jnp.float32)
            outer = jnp.einsum('sci,sdj->ijcd', left_pair, right_pair)
            outer = outer + jnp.einsum('sci,sdj->ijcd', left_free, right_free) * same_chain[:, :, None, None]
            outer_product = outer.astype(jnp.bfloat16).reshape(ref_rows * N, C * C)
            summed = summed + jnp.dot(outer_product, out_weight, preferred_element_type=jnp.float32).reshape(ref_rows, N, Z)
        denominator = S_P + same_chain * depth_block[:, None].astype(jnp.float32)
        return (summed / denominator[:, :, None] + out_bias).astype(jnp.bfloat16)

    blocks = lax.map(one_block, jnp.arange(N // ref_rows, dtype=jnp.int32))
    return blocks.reshape(N, N, Z)
```

```python
import functools

import jax
import jax.numpy as jnp
from jax import lax
from jax.experimental import pallas as pl
from jax.experimental.pallas import tpu as pltpu
from jax.sharding import PartitionSpec as P

LANES = 128
D_STEP = 8


def outer_kernel(
    paired_total, group, final,
    start_ref, end_ref, depth_ref,
    left_pair, left_free, right_pair, right_free, weight, bias,
    out_ref, outer_scr, free_scr, acc,
):
    tile, step = pl.program_id(0), pl.program_id(1)
    rows = start_ref.shape[0]
    channels = left_pair.shape[0] // rows
    width = right_pair.shape[1]
    d_step = width // LANES
    lanes = lax.broadcasted_iota(jnp.int32, (1, LANES), 1) + tile * LANES
    span = group * channels

    @pl.loop(0, rows // group)
    def _(g):
        base = g * group
        at = pl.ds(pl.multiple_of(base * channels, span), span)
        outer_scr[...] = jnp.dot(left_pair[at, :], right_pair[...], preferred_element_type=jnp.float32)
        first, last = start_ref[base], end_ref[base + group - 1]

        @pl.when((first < (tile + 1) * LANES) & (last > tile * LANES))
        def _():
            free_scr[...] = jnp.dot(left_free[at, :], right_free[...], preferred_element_type=jnp.float32)
            for i in range(group):
                same = (lanes >= start_ref[base + i]) & (lanes < end_ref[base + i])
                part = pl.ds(i * channels, channels)
                for d in range(d_step):
                    cols = pl.ds(d * LANES, LANES)
                    outer_scr[part, cols] += jnp.where(same, free_scr[part, cols], 0.0)

        for pair in range(group // 2):
            halves = []
            for i in (2 * pair, 2 * pair + 1):
                mine = outer_scr[pl.ds(i * channels, channels), :].astype(jnp.bfloat16)
                halves.append(jnp.concatenate(
                    [mine[:, d * LANES:(d + 1) * LANES] for d in range(d_step)], axis=0))
            projected = jnp.dot(
                weight[...], jnp.concatenate(halves, axis=1), preferred_element_type=jnp.float32)
            for k in range(2):
                row = base + 2 * pair + k
                value = projected[:, k * LANES:(k + 1) * LANES]

                @pl.when(step == 0)
                def _():
                    acc[row] = value

                @pl.when(step > 0)
                def _():
                    acc[row] += value

    @pl.when(step == pl.num_programs(1) - 1)
    def _():
        @pl.loop(0, rows)
        def _(i):
            same = (lanes >= start_ref[i]) & (lanes < end_ref[i])
            depth = depth_ref[i].astype(jnp.float32)
            count = paired_total + jnp.where(same, depth, 0.0)
            value = (acc[i] / count).T
            if final:
                value = value + bias[...]
            out_ref[i] = value.astype(out_ref.dtype)


def outer_product(left_pair, left_free, right_pair, right_free, weight, bias, start, end, depth, paired_total, final):
    rows = start.shape[0]
    channels = left_pair.shape[0] // rows
    out_channels = weight.shape[0]
    cols = right_pair.shape[1] // channels
    group = min(16, rows)
    width = D_STEP * LANES
    steps = channels // D_STEP
    smem = pl.BlockSpec(memory_space=pltpu.SMEM)

    def whole(x):
        return pl.BlockSpec(x.shape, lambda t, s: (0, 0))

    def streamed(x):
        return pl.BlockSpec((x.shape[0], width), lambda t, s: (0, t * steps + s))

    return pl.pallas_call(
        functools.partial(outer_kernel, float(paired_total), group, final),
        out_shape=jax.ShapeDtypeStruct((rows, cols, out_channels), jnp.bfloat16 if final else jnp.float32),
        grid=(cols // LANES, steps),
        in_specs=[
            smem, smem, smem, whole(left_pair), whole(left_free), streamed(right_pair), streamed(right_free),
            pl.BlockSpec((out_channels, D_STEP * channels), lambda t, s: (0, s)), whole(bias),
        ],
        out_specs=pl.BlockSpec((rows, LANES, out_channels), lambda t, s: (0, t, 0)),
        scratch_shapes=[
            pltpu.VMEM((group * channels, width), jnp.float32),
            pltpu.VMEM((group * channels, width), jnp.float32),
            pltpu.VMEM((rows, out_channels, LANES), jnp.float32),
        ],
        compiler_params=pltpu.CompilerParams(
            dimension_semantics=("arbitrary", "arbitrary"), vmem_limit_bytes=56 << 20),
        name="outer_product",
    )(start, end, depth, left_pair, left_free, right_pair, right_free, weight, bias)


def flat_right(x):
    depth, channels, cols = x.shape
    return x.reshape(depth, channels, cols // LANES, LANES).transpose(0, 2, 1, 3).reshape(depth, -1)


def flat_left(x):
    depth, channels, rows = x.shape
    return x.transpose(2, 1, 0).reshape(rows * channels, depth)


def body(
    paired_left, paired_right, unpaired_left, unpaired_right,
    out_weight, out_bias, chain_lengths, unpaired_depths,
):
    channels, rows = paired_left.shape[1:]
    cols = paired_right.shape[2]
    first_row = lax.axis_index("row") * rows
    first_col = lax.axis_index("col") * cols
    positions = first_row + jnp.arange(rows, dtype=jnp.int32)
    chain_ends = jnp.cumsum(chain_lengths)
    chain_starts = chain_ends - chain_lengths
    inside = (positions[:, None] >= chain_starts[None, :]) & (positions[:, None] < chain_ends[None, :])

    def pick(table):
        return jnp.sum(jnp.where(inside, table[None, :], 0), axis=1, dtype=jnp.int32)

    depth = pick(unpaired_depths)
    start = pick(chain_starts) - first_col
    end = pick(chain_ends) - first_col

    seq = lax.axis_size("seq")
    free_here = unpaired_left.shape[0]
    first_free = (lax.axis_index("seq") * lax.axis_size("col") + lax.axis_index("col")) * free_here
    free_ids = first_free + jnp.arange(free_here, dtype=jnp.int32)
    live = free_ids[:, None] < depth[None, :]
    masked = jnp.where(live[:, None, :], unpaired_left, jnp.zeros((), unpaired_left.dtype))

    right_pair = lax.all_gather(flat_right(paired_right), "row", axis=0, tiled=True)
    right_free = lax.all_gather(flat_right(unpaired_right), "row", axis=0, tiled=True)
    left_pair = lax.all_gather(flat_left(paired_left), "col", axis=1, tiled=True)
    left_free = lax.all_gather(flat_left(masked), "col", axis=1, tiled=True)

    out_channels = out_weight.shape[1]
    weight = out_weight.reshape(channels, channels, out_channels).transpose(2, 1, 0).reshape(out_channels, -1)
    bias = out_bias.reshape(1, -1)
    paired_total = right_pair.shape[0] * seq
    out = outer_product(
        left_pair, left_free, right_pair, right_free, weight, bias, start, end, depth, paired_total, seq == 1)
    if seq == 1:
        return out
    summed = lax.psum(out, "seq")
    share = cols // seq
    own = lax.dynamic_slice_in_dim(summed, lax.axis_index("seq") * share, share, 1)
    return (own + bias).astype(jnp.bfloat16)


def solution(mesh):
    return jax.shard_map(
        body,
        mesh=mesh,
        in_specs=(
            P(("groups", "seq", "col"), None, "row"),
            P(("groups", "seq", "row"), None, "col"),
            P(("groups", "seq", "col"), None, "row"),
            P(("groups", "seq", "row"), None, "col"),
            P(),
            P(),
            P("groups"),
            P("groups"),
        ),
        out_specs=P(("groups", "row"), ("col", "seq"), None),
        check_vma=False,
    )
```

```python
import functools

import jax
import jax.numpy as jnp
from jax import lax
from jax.experimental import pallas as pl
from jax.experimental.pallas import tpu as pltpu
from jax.sharding import PartitionSpec as P

LANES = 128
D_STEP = 8


def outer_kernel(
    paired_total, group, final,
    start_ref, end_ref, depth_ref,
    left_pair, left_free, right_pair, right_free, weight, bias,
    out_ref, outer_scr, free_scr, acc,
):
    tile, step = pl.program_id(0), pl.program_id(1)
    rows = start_ref.shape[0]
    channels = left_pair.shape[0] // rows
    width = right_pair.shape[1]
    d_step = width // LANES
    lanes = lax.broadcasted_iota(jnp.int32, (1, LANES), 1) + tile * LANES
    span = group * channels

    @pl.loop(0, rows // group)
    def _(g):
        base = g * group
        at = pl.ds(pl.multiple_of(base * channels, span), span)
        outer_scr[...] = jnp.dot(left_pair[at, :], right_pair[...], preferred_element_type=jnp.float32)
        first, last = start_ref[base], end_ref[base + group - 1]

        @pl.when((first < (tile + 1) * LANES) & (last > tile * LANES))
        def _():
            free_scr[...] = jnp.dot(left_free[at, :], right_free[...], preferred_element_type=jnp.float32)
            for i in range(group):
                same = (lanes >= start_ref[base + i]) & (lanes < end_ref[base + i])
                part = pl.ds(i * channels, channels)
                for d in range(d_step):
                    cols = pl.ds(d * LANES, LANES)
                    outer_scr[part, cols] += jnp.where(same, free_scr[part, cols], 0.0)

        for pair in range(group // 2):
            halves = []
            for i in (2 * pair, 2 * pair + 1):
                mine = outer_scr[pl.ds(i * channels, channels), :].astype(jnp.bfloat16)
                halves.append(jnp.concatenate(
                    [mine[:, d * LANES:(d + 1) * LANES] for d in range(d_step)], axis=0))
            projected = jnp.dot(
                weight[...], jnp.concatenate(halves, axis=1), preferred_element_type=jnp.float32)
            for k in range(2):
                row = base + 2 * pair + k
                value = projected[:, k * LANES:(k + 1) * LANES]

                @pl.when(step == 0)
                def _():
                    acc[row] = value

                @pl.when(step > 0)
                def _():
                    acc[row] += value

    @pl.when(step == pl.num_programs(1) - 1)
    def _():
        @pl.loop(0, rows)
        def _(i):
            same = (lanes >= start_ref[i]) & (lanes < end_ref[i])
            depth = depth_ref[i].astype(jnp.float32)
            count = paired_total + jnp.where(same, depth, 0.0)
            value = (acc[i] / count).T
            if final:
                value = value + bias[...]
            out_ref[i] = value.astype(out_ref.dtype)


def outer_product(left_pair, left_free, right_pair, right_free, weight, bias, start, end, depth, paired_total, final):
    rows = start.shape[0]
    channels = left_pair.shape[0] // rows
    out_channels = weight.shape[0]
    cols = right_pair.shape[1] // channels
    group = min(16, rows)
    width = D_STEP * LANES
    steps = channels // D_STEP
    smem = pl.BlockSpec(memory_space=pltpu.SMEM)

    def whole(x):
        return pl.BlockSpec(x.shape, lambda t, s: (0, 0))

    def streamed(x):
        return pl.BlockSpec((x.shape[0], width), lambda t, s: (0, t * steps + s))

    return pl.pallas_call(
        functools.partial(outer_kernel, float(paired_total), group, final),
        out_shape=jax.ShapeDtypeStruct((rows, cols, out_channels), jnp.bfloat16 if final else jnp.float32),
        grid=(cols // LANES, steps),
        in_specs=[
            smem, smem, smem, whole(left_pair), whole(left_free), streamed(right_pair), streamed(right_free),
            pl.BlockSpec((out_channels, D_STEP * channels), lambda t, s: (0, s)), whole(bias),
        ],
        out_specs=pl.BlockSpec((rows, LANES, out_channels), lambda t, s: (0, t, 0)),
        scratch_shapes=[
            pltpu.VMEM((group * channels, width), jnp.float32),
            pltpu.VMEM((group * channels, width), jnp.float32),
            pltpu.VMEM((rows, out_channels, LANES), jnp.float32),
        ],
        compiler_params=pltpu.CompilerParams(
            dimension_semantics=("arbitrary", "arbitrary"), vmem_limit_bytes=56 << 20),
        name="outer_product",
    )(start, end, depth, left_pair, left_free, right_pair, right_free, weight, bias)


def flat_right(x):
    depth, channels, cols = x.shape
    return x.reshape(depth, channels, cols // LANES, LANES).transpose(0, 2, 1, 3).reshape(depth, -1)


def flat_left(x):
    depth, channels, rows = x.shape
    return x.transpose(2, 1, 0).reshape(rows * channels, depth)


MESH = pl.DeviceIdType.MESH
Y_SIZE, CORES = 2, 2


def gather_kernel(depth, width, pair_in, free_in, left_pair_in, left_free_in, pair_out, free_out, left_pair_out,
                  left_free_out, send_sem, recv_sem, left_send, left_recv, local_sem):
    row, col = lax.axis_index("row"), lax.axis_index("col")
    core, y, z = row % CORES, (row // CORES) % Y_SIZE, row // (CORES * Y_SIZE)

    def row_of(z_at, y_at, core_at):
        return (z_at * Y_SIZE + y_at) * CORES + core_at

    up, down = row_of(z + 1, y, core), row_of(z - 1, y, core)
    across, sibling = row_of(z, 1 - y, core), row_of(z, y, 1 - core)
    has_up, has_down = z < depth - 1, z > 0

    barrier = pltpu.get_barrier_semaphore()

    def greet(axis, at):
        pl.semaphore_signal(barrier, inc=1, device_id={axis: at}, device_id_type=MESH)

    pl.when(has_up)(lambda: greet("row", up))
    pl.when(has_down)(lambda: greet("row", down))
    greet("row", across)
    greet("row", sibling)
    for shift in range(1, width):
        greet("col", lax.rem(col + shift, width))
    pl.semaphore_wait(barrier, jnp.where(has_up, 1, 0) + jnp.where(has_down, 1, 0) + 2 + width - 1)

    pieces = [(pair_in, pair_out, 0), (free_in, free_out, 0), (free_in, free_out, 1), (pair_in, pair_out, 1)]
    early = {0}

    def copy(piece, way, origin, target, own):
        source, out, half = pieces[piece]
        here = out.at[origin, half]
        return pltpu.make_async_remote_copy(
            src_ref=source.at[half] if own else here, dst_ref=here,
            send_sem=send_sem.at[way, piece, origin // CORES], recv_sem=recv_sem.at[piece, origin],
            device_id={"row": target}, device_id_type=MESH)

    def forward(piece, z_at, y_at, started):
        origin = row_of(z_at, y_at, core)
        own_line = y_at is y
        own = own_line and z_at is z
        def go(way, target):
            c = copy(piece, way, origin, target, own)
            c.start() if started else c.wait_send()
        if own_line or piece in early:
            pl.when(has_up & (z_at <= z))(lambda: go(0, up))
            pl.when(has_down & (z_at >= z))(lambda: go(1, down))
        if own_line and (own or piece not in early):
            go(2, across)
        go(3, sibling)

    def arrive(piece, z_at, y_at, core_at):
        origin = row_of(z_at, y_at, core_at)
        copy(piece, 3, origin, sibling, False).wait_recv()

    for piece in range(len(pieces)):
        forward(piece, z, y, True)

    lefts = [(left_pair_in, left_pair_out), (left_free_in, left_free_out)]
    left_copies = []
    for n, (source, out) in enumerate(lefts):
        for shift in range(1, width):
            c = pltpu.make_async_remote_copy(
                src_ref=source, dst_ref=out.at[col], send_sem=left_send.at[n, shift], recv_sem=left_recv.at[n, shift],
                device_id={"col": lax.rem(col + shift, width)}, device_id_type=MESH)
            c.start()
            left_copies.append(c)
    local = [
        pltpu.make_async_copy(pair_in, pair_out.at[row], local_sem.at[0]),
        pltpu.make_async_copy(free_in, free_out.at[row], local_sem.at[1]),
        pltpu.make_async_copy(left_pair_in, left_pair_out.at[col], local_sem.at[2]),
        pltpu.make_async_copy(left_free_in, left_free_out.at[col], local_sem.at[3]),
    ]
    for c in local:
        c.start()

    other = 1 - y

    def hops(hop):
        if hop == 0:
            return ((z, None),)
        return ((z - hop, z >= hop), (z + hop, z + hop < depth))

    def sweep(hop, y_at):
        for piece in range(len(pieces)):
            for z_at, there in hops(hop):
                def step(piece=piece, z_at=z_at):
                    arrive(piece, z_at, y_at, core)
                    forward(piece, z_at, y_at, True)
                step() if there is None else pl.when(there)(step)

    for hop in range(depth):
        if hop > 0:
            sweep(hop, y)
        sweep(hop, other)

    def every(do):
        for piece in range(len(pieces)):
            for hop in range(depth):
                for z_at, there in hops(hop):
                    for y_at in (y, other):
                        step = functools.partial(do, piece, z_at, y_at)
                        step() if there is None else pl.when(there)(step)

    every(lambda piece, z_at, y_at: arrive(piece, z_at, y_at, 1 - core))
    every(lambda piece, z_at, y_at: forward(piece, z_at, y_at, False))
    for c in left_copies:
        c.wait()
    for c in local:
        c.wait()


def gather_all(right_pair, right_free, left_pair, left_free):
    count, width = lax.axis_size("row"), lax.axis_size("col")
    depth = count // (Y_SIZE * CORES)

    def halved(x):
        return x.reshape(2, x.shape[0] // 2, x.shape[1])

    ins = (halved(right_pair), halved(right_free), left_pair, left_free)
    counts = (count, count, width, width)
    outs = pl.pallas_call(
        functools.partial(gather_kernel, depth, width),
        out_shape=[jax.ShapeDtypeStruct((n,) + x.shape, x.dtype) for n, x in zip(counts, ins)],
        in_specs=[pl.BlockSpec(memory_space=pl.ANY)] * 4,
        out_specs=[pl.BlockSpec(memory_space=pl.ANY)] * 4,
        scratch_shapes=[
            pltpu.SemaphoreType.DMA((4, 4, count // CORES)),
            pltpu.SemaphoreType.DMA((4, count)),
            pltpu.SemaphoreType.DMA((2, width)),
            pltpu.SemaphoreType.DMA((2, width)),
            pltpu.SemaphoreType.DMA((4,)),
        ],
        compiler_params=pltpu.CompilerParams(collective_id=0, has_side_effects=True),
        name="gather_all",
    )(*ins)
    right = [x.reshape(-1, x.shape[-1]) for x in outs[:2]]
    left = [x.transpose(1, 0, 2).reshape(x.shape[1], -1) for x in outs[2:]]
    return (*right, *left)


def body(
    paired_left, paired_right, unpaired_left, unpaired_right,
    out_weight, out_bias, chain_lengths, unpaired_depths,
):
    channels, rows = paired_left.shape[1:]
    cols = paired_right.shape[2]
    first_row = lax.axis_index("row") * rows
    first_col = lax.axis_index("col") * cols
    positions = first_row + jnp.arange(rows, dtype=jnp.int32)
    chain_ends = jnp.cumsum(chain_lengths)
    chain_starts = chain_ends - chain_lengths
    inside = (positions[:, None] >= chain_starts[None, :]) & (positions[:, None] < chain_ends[None, :])

    def pick(table):
        return jnp.sum(jnp.where(inside, table[None, :], 0), axis=1, dtype=jnp.int32)

    depth = pick(unpaired_depths)
    start = pick(chain_starts) - first_col
    end = pick(chain_ends) - first_col

    seq = lax.axis_size("seq")
    free_here = unpaired_left.shape[0]
    first_free = (lax.axis_index("seq") * lax.axis_size("col") + lax.axis_index("col")) * free_here
    free_ids = first_free + jnp.arange(free_here, dtype=jnp.int32)
    live = free_ids[:, None] < depth[None, :]
    masked = jnp.where(live[:, None, :], unpaired_left, jnp.zeros((), unpaired_left.dtype))

    right_pair, right_free, left_pair, left_free = gather_all(
        flat_right(paired_right), flat_right(unpaired_right), flat_left(paired_left), flat_left(masked))

    out_channels = out_weight.shape[1]
    weight = out_weight.reshape(channels, channels, out_channels).transpose(2, 1, 0).reshape(out_channels, -1)
    bias = out_bias.reshape(1, -1)
    paired_total = right_pair.shape[0] * seq
    out = outer_product(
        left_pair, left_free, right_pair, right_free, weight, bias, start, end, depth, paired_total, seq == 1)
    if seq == 1:
        return out
    summed = lax.psum(out, "seq")
    share = cols // seq
    own = lax.dynamic_slice_in_dim(summed, lax.axis_index("seq") * share, share, 1)
    return (own + bias).astype(jnp.bfloat16)


def solution(mesh):
    return jax.shard_map(
        body,
        mesh=mesh,
        in_specs=(
            P(("groups", "seq", "col"), None, "row"),
            P(("groups", "seq", "row"), None, "col"),
            P(("groups", "seq", "col"), None, "row"),
            P(("groups", "seq", "row"), None, "col"),
            P(),
            P(),
            P("groups"),
            P("groups"),
        ),
        out_specs=P(("groups", "row"), ("col", "seq"), None),
        check_vma=False,
    )
```

```python
import functools

import jax
import jax.numpy as jnp
from jax import lax
from jax.experimental import pallas as pl
from jax.experimental.pallas import tpu as pltpu
from jax.sharding import PartitionSpec as P

LANES = 128
D_STEP = 16


def outer_kernel(
    paired_total, group, final,
    start_ref, end_ref, depth_ref,
    left_pair, left_free, right_pair, right_free, weight, bias,
    out_ref, outer_scr, free_scr, acc,
):
    tile, step = pl.program_id(0), pl.program_id(1)
    rows = start_ref.shape[0]
    channels = left_pair.shape[1] // rows
    width = right_pair.shape[1]
    d_step = width // LANES
    lanes = lax.broadcasted_iota(jnp.int32, (1, LANES), 1) + tile * LANES
    span = group * channels

    @pl.when(step == 0)
    def _():
        acc[...] = jnp.zeros_like(acc)

    def left(ref, at):
        return jnp.concatenate([ref[n, at, :] for n in range(ref.shape[0])], axis=1)

    @pl.loop(0, rows // group)
    def _(g):
        base = g * group
        at = pl.ds(pl.multiple_of(base * channels, span), span)
        outer_scr[...] = jnp.dot(left(left_pair, at), right_pair[...], preferred_element_type=jnp.float32)
        first, last = start_ref[base], end_ref[base + group - 1]

        @pl.when((first < (tile + 1) * LANES) & (last > tile * LANES))
        def _():
            free_scr[...] = jnp.dot(left(left_free, at), right_free[...], preferred_element_type=jnp.float32)
            for i in range(group):
                same = (lanes >= start_ref[base + i]) & (lanes < end_ref[base + i])
                part = pl.ds(i * channels, channels)
                for d in range(d_step):
                    cols = pl.ds(d * LANES, LANES)
                    outer_scr[part, cols] += jnp.where(same, free_scr[part, cols], 0.0)

        for pair in range(group // 2):
            halves = []
            for i in (2 * pair, 2 * pair + 1):
                mine = outer_scr[pl.ds(i * channels, channels), :].astype(jnp.bfloat16)
                halves.append(jnp.concatenate(
                    [mine[:, d * LANES:(d + 1) * LANES] for d in range(d_step)], axis=0))
            projected = jnp.dot(
                weight[...], jnp.concatenate(halves, axis=1), preferred_element_type=jnp.float32)
            for k in range(2):
                acc[base + 2 * pair + k] += projected[:, k * LANES:(k + 1) * LANES]

    @pl.when(step == pl.num_programs(1) - 1)
    def _():
        @pl.loop(0, rows)
        def _(i):
            same = (lanes >= start_ref[i]) & (lanes < end_ref[i])
            depth = depth_ref[i].astype(jnp.float32)
            count = paired_total + jnp.where(same, depth, 0.0)
            value = (acc[i] * (1.0 / count)).T
            if final:
                value = value + bias[...]
            out_ref[i] = value.astype(out_ref.dtype)


def outer_product(left_pair, left_free, right_pair, right_free, weight, bias, start, end, depth, paired_total, final):
    rows = start.shape[0]
    channels = left_pair.shape[1] // rows
    out_channels = weight.shape[0]
    cols = right_pair.shape[1] // channels
    group = min(16, rows)
    width = D_STEP * LANES
    steps = channels // D_STEP
    smem = pl.BlockSpec(memory_space=pltpu.SMEM)

    def whole(x):
        return pl.BlockSpec(x.shape, lambda t, s: (0,) * x.ndim)

    def streamed(x):
        return pl.BlockSpec((x.shape[0], width), lambda t, s: (0, t * steps + s))

    return pl.pallas_call(
        functools.partial(outer_kernel, float(paired_total), group, final),
        out_shape=jax.ShapeDtypeStruct((rows, cols, out_channels), jnp.bfloat16 if final else jnp.float32),
        grid=(cols // LANES, steps),
        in_specs=[
            smem, smem, smem, whole(left_pair), whole(left_free), streamed(right_pair), streamed(right_free),
            pl.BlockSpec((out_channels, D_STEP * channels), lambda t, s: (0, s)), whole(bias),
        ],
        out_specs=pl.BlockSpec((rows, LANES, out_channels), lambda t, s: (0, t, 0)),
        scratch_shapes=[
            pltpu.VMEM((group * channels, width), jnp.float32),
            pltpu.VMEM((group * channels, width), jnp.float32),
            pltpu.VMEM((rows, out_channels, LANES), jnp.float32),
        ],
        compiler_params=pltpu.CompilerParams(
            dimension_semantics=("arbitrary", "arbitrary"), vmem_limit_bytes=56 << 20),
        name="outer_product",
    )(start, end, depth, left_pair, left_free, right_pair, right_free, weight, bias)


def flat_right(x):
    depth, channels, cols = x.shape
    return x.reshape(depth, channels, cols // LANES, LANES).transpose(0, 2, 1, 3).reshape(depth, -1)


def flat_left(x):
    depth, channels, rows = x.shape
    return x.transpose(2, 1, 0).reshape(rows * channels, depth)


MESH = pl.DeviceIdType.MESH
Y_SIZE, CORES = 2, 2


def gather_kernel(depth, width, pair_in, free_in, left_pair_in, left_free_in, pair_out, free_out, left_pair_out,
                  left_free_out, send_sem, recv_sem, left_send, left_recv, local_sem):
    row, col = lax.axis_index("row"), lax.axis_index("col")
    core, y, z = row % CORES, (row // CORES) % Y_SIZE, row // (CORES * Y_SIZE)

    def row_of(z_at, y_at, core_at):
        return (z_at * Y_SIZE + y_at) * CORES + core_at

    up, down = row_of(z + 1, y, core), row_of(z - 1, y, core)
    across, sibling = row_of(z, 1 - y, core), row_of(z, y, 1 - core)
    has_up, has_down = z < depth - 1, z > 0

    barrier = pltpu.get_barrier_semaphore()

    def greet(axis, at):
        pl.semaphore_signal(barrier, inc=1, device_id={axis: at}, device_id_type=MESH)

    pl.when(has_up)(lambda: greet("row", up))
    pl.when(has_down)(lambda: greet("row", down))
    greet("row", across)
    greet("row", sibling)
    for shift in range(1, width):
        greet("col", lax.rem(col + shift, width))
    pl.semaphore_wait(barrier, jnp.where(has_up, 1, 0) + jnp.where(has_down, 1, 0) + 2 + width - 1)

    pieces = [(pair_in, pair_out, 0), (free_in, free_out, 0), (free_in, free_out, 1), (pair_in, pair_out, 1)]
    early = {0}

    def copy(piece, way, origin, target, own):
        source, out, half = pieces[piece]
        here = out.at[origin, half]
        return pltpu.make_async_remote_copy(
            src_ref=source.at[half] if own else here, dst_ref=here,
            send_sem=send_sem.at[way, piece, origin // CORES], recv_sem=recv_sem.at[piece, origin],
            device_id={"row": target}, device_id_type=MESH)

    def forward(piece, z_at, y_at, started):
        origin = row_of(z_at, y_at, core)
        own_line = y_at is y
        own = own_line and z_at is z
        def go(way, target):
            c = copy(piece, way, origin, target, own)
            c.start() if started else c.wait_send()
        if own_line or piece in early:
            pl.when(has_up & (z_at <= z))(lambda: go(0, up))
            pl.when(has_down & (z_at >= z))(lambda: go(1, down))
        if own_line and (own or piece not in early):
            go(2, across)
        go(3, sibling)

    def arrive(piece, z_at, y_at, core_at):
        origin = row_of(z_at, y_at, core_at)
        copy(piece, 3, origin, sibling, False).wait_recv()

    for piece in range(len(pieces)):
        forward(piece, z, y, True)

    lefts = [(left_pair_in, left_pair_out), (left_free_in, left_free_out)]
    left_copies = []
    for n, (source, out) in enumerate(lefts):
        for shift in range(1, width):
            c = pltpu.make_async_remote_copy(
                src_ref=source, dst_ref=out.at[col], send_sem=left_send.at[n, shift], recv_sem=left_recv.at[n, shift],
                device_id={"col": lax.rem(col + shift, width)}, device_id_type=MESH)
            c.start()
            left_copies.append(c)
    local = [
        pltpu.make_async_copy(pair_in, pair_out.at[row], local_sem.at[0]),
        pltpu.make_async_copy(free_in, free_out.at[row], local_sem.at[1]),
        pltpu.make_async_copy(left_pair_in, left_pair_out.at[col], local_sem.at[2]),
        pltpu.make_async_copy(left_free_in, left_free_out.at[col], local_sem.at[3]),
    ]
    for c in local:
        c.start()

    other = 1 - y

    def hops(hop):
        if hop == 0:
            return ((z, None),)
        return ((z - hop, z >= hop), (z + hop, z + hop < depth))

    def sweep(hop, y_at):
        for piece in range(len(pieces)):
            for z_at, there in hops(hop):
                def step(piece=piece, z_at=z_at):
                    arrive(piece, z_at, y_at, core)
                    forward(piece, z_at, y_at, True)
                step() if there is None else pl.when(there)(step)

    for hop in range(depth):
        if hop > 0:
            sweep(hop, y)
        sweep(hop, other)

    def every(do):
        for piece in range(len(pieces)):
            for hop in range(depth):
                for z_at, there in hops(hop):
                    for y_at in (y, other):
                        step = functools.partial(do, piece, z_at, y_at)
                        step() if there is None else pl.when(there)(step)

    every(lambda piece, z_at, y_at: arrive(piece, z_at, y_at, 1 - core))
    every(lambda piece, z_at, y_at: forward(piece, z_at, y_at, False))
    for c in left_copies:
        c.wait()
    for c in local:
        c.wait()


def gather_all(right_pair, right_free, left_pair, left_free):
    count, width = lax.axis_size("row"), lax.axis_size("col")
    depth = count // (Y_SIZE * CORES)

    def halved(x):
        return x.reshape(2, x.shape[0] // 2, x.shape[1])

    ins = (halved(right_pair), halved(right_free), left_pair, left_free)
    counts = (count, count, width, width)
    outs = pl.pallas_call(
        functools.partial(gather_kernel, depth, width),
        out_shape=[jax.ShapeDtypeStruct((n,) + x.shape, x.dtype) for n, x in zip(counts, ins)],
        in_specs=[pl.BlockSpec(memory_space=pl.ANY)] * 4,
        out_specs=[pl.BlockSpec(memory_space=pl.ANY)] * 4,
        scratch_shapes=[
            pltpu.SemaphoreType.DMA((4, 4, count // CORES)),
            pltpu.SemaphoreType.DMA((4, count)),
            pltpu.SemaphoreType.DMA((2, width)),
            pltpu.SemaphoreType.DMA((2, width)),
            pltpu.SemaphoreType.DMA((4,)),
        ],
        compiler_params=pltpu.CompilerParams(collective_id=0, has_side_effects=True),
        name="gather_all",
    )(*ins)
    right = [x.reshape(-1, x.shape[-1]) for x in outs[:2]]
    return (*right, *outs[2:])


def body(
    paired_left, paired_right, unpaired_left, unpaired_right,
    out_weight, out_bias, chain_lengths, unpaired_depths,
):
    channels, rows = paired_left.shape[1:]
    cols = paired_right.shape[2]
    first_row = lax.axis_index("row") * rows
    first_col = lax.axis_index("col") * cols
    positions = first_row + jnp.arange(rows, dtype=jnp.int32)
    chains = jnp.arange(chain_lengths.shape[0])
    chain_ends = jnp.sum(
        jnp.where(chains[None, :] <= chains[:, None], chain_lengths[None, :], 0), axis=1, dtype=jnp.int32)
    chain_starts = chain_ends - chain_lengths
    inside = (positions[:, None] >= chain_starts[None, :]) & (positions[:, None] < chain_ends[None, :])

    def pick(table):
        return jnp.sum(jnp.where(inside, table[None, :], 0), axis=1, dtype=jnp.int32)

    depth = pick(unpaired_depths)
    start = pick(chain_starts) - first_col
    end = pick(chain_ends) - first_col

    seq = lax.axis_size("seq")
    free_here = unpaired_left.shape[0]
    first_free = (lax.axis_index("seq") * lax.axis_size("col") + lax.axis_index("col")) * free_here
    free_ids = first_free + jnp.arange(free_here, dtype=jnp.int32)
    live = free_ids[:, None] < depth[None, :]
    masked = jnp.where(live[:, None, :], unpaired_left, jnp.zeros((), unpaired_left.dtype))

    right_pair, right_free, left_pair, left_free = gather_all(
        flat_right(paired_right), flat_right(unpaired_right), flat_left(paired_left), flat_left(masked))

    out_channels = out_weight.shape[1]
    weight = out_weight.reshape(channels, channels, out_channels).transpose(2, 1, 0).reshape(out_channels, -1)
    bias = out_bias.reshape(1, -1)
    paired_total = right_pair.shape[0] * seq
    out = outer_product(
        left_pair, left_free, right_pair, right_free, weight, bias, start, end, depth, paired_total, seq == 1)
    if seq == 1:
        return out
    summed = lax.psum(out, "seq")
    share = cols // seq
    own = lax.dynamic_slice_in_dim(summed, lax.axis_index("seq") * share, share, 1)
    return (own + bias).astype(jnp.bfloat16)


def solution(mesh):
    return jax.shard_map(
        body,
        mesh=mesh,
        in_specs=(
            P(("groups", "seq", "col"), None, "row"),
            P(("groups", "seq", "row"), None, "col"),
            P(("groups", "seq", "col"), None, "row"),
            P(("groups", "seq", "row"), None, "col"),
            P(),
            P(),
            P("groups"),
            P("groups"),
        ),
        out_specs=P(("groups", "row"), ("col", "seq"), None),
        check_vma=False,
    )
```
